16 devices in a mesh: dp: 1, sp: 16 (over x, y, z, core).
Axes of the slice: x: 2, y: 2, z: 2, core: 2. Of those that a mesh axis runs over, the one named last changes fastest.
Arguments:
- x: bfloat16 [2048, 6144], P(('dp', 'sp'))
- gain: bfloat16 [6144], replicated
- wq: bfloat16 [6144, 6144], replicated
- wk: bfloat16 [6144, 1024], replicated
- wv: bfloat16 [6144, 1024], replicated
- wo: bfloat16 [6144, 6144], replicated
Outputs:
- output: bfloat16 [2048, 6144], P(('dp', 'sp'))
All inputs are finite; a program needn't handle non-finite values.
Results may differ from the reference program's by a relative error of at most 0.012.
Values are sent between devices in bfloat16 or wider.
A program may use at most 2 GiB of HBM per device.

```python
import jax
import jax.numpy as jnp
from jax import lax

ROWS = 2048
D = 6144
HEADS = 48
KV_HEADS = 8
HEAD = 128
THETA = 10000


def setup_inputs(seed: int = 0, part: int = 0) -> dict:
    kx, kn, kq, kk, kv, ko = jax.random.split(jax.random.key(seed), 6)

    def weights(key, rows, columns):
        return jax.random.normal(key, (rows, columns), jnp.float32) * rows**-0.5

    drawn = {
        "x": jax.random.normal(jax.random.fold_in(kx, part), (ROWS, D), jnp.float32),
        "gain": 1 + 0.1 * jax.random.normal(kn, (D,), jnp.float32),
        "wq": 2 * weights(kq, D, HEADS * HEAD),
        "wk": 2 * weights(kk, D, KV_HEADS * HEAD),
        "wv": 4 * weights(kv, D, KV_HEADS * HEAD),
        "wo": weights(ko, HEADS * HEAD, D),
    }
    return {k: v.astype(jnp.bfloat16) for k, v in drawn.items()}


def normed(x, gain):
    wide = x.astype(jnp.float32)
    scale = lax.rsqrt(jnp.mean(wide * wide, -1, keepdims=True) + 1e-6)
    return (wide * scale * gain.astype(jnp.float32)).astype(jnp.bfloat16)


def turned(t, place, theta):
    half = t.shape[-1] // 2
    angle = place.astype(jnp.float32)[:, None] * theta ** (-jnp.arange(half, dtype=jnp.float32) / half)
    cos, sin = jnp.cos(angle)[:, None], jnp.sin(angle)[:, None]
    a, b = t[..., :half].astype(jnp.float32), t[..., half:].astype(jnp.float32)
    return jnp.concatenate([a * cos - b * sin, b * cos + a * sin], -1).astype(jnp.bfloat16)


def matmul(a, w):
    return jnp.dot(a, w, preferred_element_type=jnp.float32).astype(jnp.bfloat16)


def einsum(form, a, b):
    return jnp.einsum(form, a.astype(jnp.float32), b.astype(jnp.float32))


def attention(q, k, v):
    scores = einsum("tgsd,ugd->gstu", q, k) * q.shape[-1] ** -0.5
    token = jnp.arange(q.shape[0])
    scores = jnp.where(token[:, None] >= token, scores, -jnp.inf)
    weights = jax.nn.softmax(scores, -1).astype(jnp.bfloat16)
    return einsum("gstu,ugd->tgsd", weights, v).astype(jnp.bfloat16)


def reference(x, gain, wq, wk, wv, wo):
    a, place = normed(x, gain), jnp.arange(ROWS)
    q = turned(matmul(a, wq).reshape(ROWS, HEADS, HEAD), place, THETA).reshape(ROWS, KV_HEADS, -1, HEAD)
    k = turned(matmul(a, wk).reshape(ROWS, KV_HEADS, HEAD), place, THETA)
    v = matmul(a, wv).reshape(ROWS, KV_HEADS, HEAD)
    seen = attention(q, k, v).reshape(ROWS, HEADS * HEAD)
    return (x.astype(jnp.float32) + jnp.dot(seen, wo, preferred_element_type=jnp.float32)).astype(jnp.bfloat16)
```

```python
import functools

import jax
import jax.numpy as jnp
import numpy as np
from jax import lax
from jax.experimental import pallas as pl
from jax.experimental.pallas import tpu as pltpu
from jax.sharding import PartitionSpec as P

MESH = pl.DeviceIdType.MESH
HEAD = 128
THETA = 10000
NEG = -1e30
LOG2E = 1.4426950408889634
E = HEAD**-0.5 * LOG2E

OWN = 128
CHIP = 2 * OWN
D = 6144
CHIPS = 8
Q_HEADS, KV_HEADS = 24, 4
GROUP = Q_HEADS // KV_HEADS
COLS = GROUP * CHIP
WIDE = 512
SLOTS = 12
NARROW = 256
HALF = D // 2
KVW = KV_HEADS * HEAD
PIECES = ((0, 96), (96, 80), (176, 80))


def _dot(a, b, ca, cb):
    return lax.dot_general(a, b, (((ca,), (cb,)), ((), ())), preferred_element_type=jnp.float32)


def _xor(m, d):
    return sum(b * ((m // b) % 2 + (d // b) % 2 - 2 * ((m // b) % 2) * ((d // b) % 2)) for b in (1, 2, 4))


def _kernel(x_ref, gain_ref, turn_ref, wq_ref, wk_ref, wv_ref, wo_ref, y_ref,
            w_s, a_s, x_s, gain_s, cos_s, sin_s, kv_s, q_s, mix_s, top_s, acc_s, got_s, out_s,
            w_sem, x_sem, t_sem, a_send, a_recv, kv_send, kv_recv, o_send, o_recv, y_sem):
    me = lax.axis_index("sp")
    chip, core = me // 2, me % 2
    mate = 2 * chip + 1 - core
    nx, ny, nz = (_xor(chip, d) for d in (4, 2, 1))

    def load(i):
        slot = i % SLOTS
        if i < 16:
            ref, col = ((wk_ref, core * KVW + NARROW * i) if i < 2 else (wv_ref, core * KVW + NARROW * (i - 2)) if i < 4
                        else (wq_ref, core * HALF + NARROW * (i - 4)))
            col = pl.multiple_of(col, 128)
            return [pltpu.make_async_copy(ref.at[pl.ds(HALF * k, HALF), pl.ds(col, NARROW)],
                                          w_s.at[slot, pl.ds(HALF * k, HALF), :], w_sem.at[slot, k]) for k in range(2)]
        n = i - 16
        row = pl.multiple_of(core * HALF, 128)
        return [pltpu.make_async_copy(wo_ref.at[pl.ds(row, HALF), pl.ds(2 * NARROW * n + NARROW * k, NARROW)],
                                      w_s.at[slot, pl.ds(HALF * k, HALF), :], w_sem.at[slot, k]) for k in range(2)]

    def fetch(i):
        for copy in load(i):
            copy.start()

    def ready(slot):
        for k in range(2):
            pltpu.make_async_copy(wo_ref.at[pl.ds(0, HALF), pl.ds(0, NARROW)], w_s.at[slot, pl.ds(HALF * k, HALF), :],
                                  w_sem.at[slot, k]).wait()

    rows = D // 192
    def x_copy(i):
        return pltpu.make_async_copy(x_ref.at[pl.ds(rows * i, rows), :], x_s.at[pl.ds(rows * i, rows), :], x_sem.at[i])

    place = pl.multiple_of(chip * CHIP, CHIP)
    tables = [pltpu.make_async_copy(gain_ref, gain_s, t_sem.at[0]),
              pltpu.make_async_copy(turn_ref.at[pl.ds(place, CHIP), :], cos_s, t_sem.at[1])]
    tables[0].start()
    for i in range(OWN // rows):
        x_copy(i).start()
    for t in tables[1:]:
        t.start()
    for i in range(SLOTS):
        fetch(i)

    barrier = pltpu.get_barrier_semaphore()
    for to in (mate, 2 * nx + core, 2 * ny + core, 2 * nz + core):
        pl.semaphore_signal(barrier, inc=1, device_id={"sp": to}, device_id_type=MESH)
    pl.semaphore_wait(barrier, 4)

    def a_copy(i, first):
        part = pl.ds(pl.multiple_of(first + rows * i, rows), rows)
        return pltpu.make_async_remote_copy(src_ref=a_s.at[part, :], dst_ref=a_s.at[part, :], send_sem=a_send.at[i], recv_sem=a_recv.at[i],
                                            device_id={"sp": mate}, device_id_type=MESH)

    tables[0].wait()

    def norm(i, _):
        x_copy(i).wait()
        wide = x_s[pl.ds(pl.multiple_of(rows * i, rows), rows), :].astype(jnp.float32)
        scale = lax.rsqrt(jnp.mean(wide * wide, -1, keepdims=True) + 1e-6)
        a_s[pl.ds(pl.multiple_of(OWN * core + rows * i, rows), rows), :] = (wide * scale * gain_s[...]).astype(jnp.bfloat16)
        a_copy(i, OWN * core).start()

    lax.fori_loop(0, OWN // rows, norm, None)
    for t in tables[1:]:
        t.wait()
    for i in range(OWN // rows):
        a_copy(i, OWN * (1 - core)).wait_recv()
        a_copy(i, OWN * core).wait_send()
    low = lax.broadcasted_iota(jnp.int32, (CHIP, HEAD), 1) < HEAD // 2
    other_half = pltpu.roll(cos_s[...], HEAD // 2, 1)
    sin_s[...] = jnp.where(low, -other_half, cos_s[...])
    cos_s[...] = jnp.where(low, cos_s[...], other_half)

    def turned(t):
        t = t.astype(jnp.bfloat16).astype(jnp.float32)
        return (t * cos_s[...] + pltpu.roll(t, HEAD // 2, 1) * sin_s[...]).astype(jnp.bfloat16)

    for i in range(4):
        ready(i)
    for i in range(4):
        t = _dot(a_s[...], w_s[i], 1, 0)
        for n in range(2):
            head = t[:, HEAD * n : HEAD * n + HEAD]
            kv_s[chip, :, NARROW * i + HEAD * n : NARROW * i + HEAD * n + HEAD] = turned(head) if i < 2 else head.astype(jnp.bfloat16)
    for i in range(4):
        fetch(SLOTS + i)

    def kv_copy(source, p, to, sem):
        part = pl.ds(PIECES[p][0], PIECES[p][1])
        return pltpu.make_async_remote_copy(src_ref=kv_s.at[source, part, :], dst_ref=kv_s.at[source, part, :], send_sem=kv_send.at[sem],
                                            recv_sem=kv_recv.at[source, p], device_id={"sp": 2 * to + core}, device_id_type=MESH)

    def arrived(source, p):
        kv_copy(source, p, nx, 0).wait_recv()

    sent = []

    def send(source, p, to):
        copy = kv_copy(source, p, to, len(sent))
        copy.start()
        sent.append(copy)

    for k in range(3):
        for at, to in enumerate((nx, ny, nz)):
            send(chip, (at + k) % 3, to)

    def forward(k):
        for at, (source, to) in enumerate(((nx, ny), (ny, nz), (nz, nx))):
            arrived(source, (at + k) % 3)
            send(source, (at + k) % 3, to)

    def queries(t):
        first = (4 + 4 * t) % SLOTS
        for u in range(4):
            ready(first + u)
        for u in range(4):
            got = _dot(a_s[...], w_s[first + u], 1, 0)
            for n in range(2):
                q_s[8 * t + 2 * u + n] = turned(got[:, HEAD * n : HEAD * n + HEAD])

    queries(0)
    for i in range(4):
        fetch(16 + i)
    queries(1)
    for i in range(4):
        fetch(20 + i)
    forward(0)
    queries(2)
    for i in range(4):
        fetch(24 + i)
    forward(1)

    ones = jnp.ones((8, CHIP), jnp.bfloat16)

    def block(source, own):
        for h in range(KV_HEADS):
            keys = kv_s[source, :, HEAD * h : HEAD * h + HEAD]
            values = jnp.concatenate([kv_s[source, :, KVW + HEAD * h : KVW + HEAD * h + HEAD].T, ones], axis=0)
            q = q_s[GROUP * h : GROUP * h + GROUP].reshape(COLS, HEAD)
            for at in range(0, COLS, WIDE):
                here = slice(at, at + WIDE)
                s = _dot(keys, q[here], 1, 1)
                if own:
                    query = lax.broadcasted_iota(jnp.int32, s.shape, 1) % CHIP
                    s = jnp.where(query >= lax.broadcasted_iota(jnp.int32, s.shape, 0), s, 2 * NEG)
                    top = s.max(axis=0, keepdims=True)
                    top_s[h, :, here] = top
                    mix_s[h, :, here] = _dot(values, jnp.exp2((s - top) * E).astype(jnp.bfloat16), 1, 0)
                else:
                    old = top_s[h, :, here]
                    top = jnp.maximum(old, s.max(axis=0, keepdims=True))
                    top_s[h, :, here] = top
                    p = jnp.exp2((s - top) * E).astype(jnp.bfloat16)
                    mix_s[h, :, here] = mix_s[h, :, here] * jnp.exp2((old - top) * E) + _dot(values, p, 1, 0)

    block(chip, True)
    forward(2)

    def other(i, _):
        source = _xor(chip, i + 1 + i // 2 - 2 * (i // 3) + i // 6)

        @pl.when(source < chip)
        def _():
            block(source, False)

    far = [(_xor(chip, 6), 0, nz), (_xor(chip, 3), 1, nx), (_xor(chip, 5), 2, ny)]
    last = _xor(chip, 7)
    def step(i, _):
        @pl.when(i == 3)
        def _():
            for source, p, to in far:
                arrived(source, p)
                kv_copy(source, p, to, 18 + p).start()
            for source, p, to in far:
                for other_p in range(3):
                    if other_p != p:
                        arrived(source, other_p)

        @pl.when(i == 6)
        def _():
            for p in range(3):
                arrived(last, p)

        other(i, None)

    lax.fori_loop(0, 7, step, None)
    for source, p, to in far:
        sent.append(kv_copy(source, p, to, 18 + p))

    for h in range(KV_HEADS):
        for g in range(GROUP):
            here = slice(g * CHIP, g * CHIP + CHIP)
            seen = mix_s[h, :HEAD, here] * (1 / mix_s[h, HEAD : HEAD + 1, here])
            n = GROUP * h + g
            a_s[:, HEAD * n : HEAD * n + HEAD] = seen.T.astype(jnp.bfloat16)

    own_rows = pl.ds(pl.multiple_of(OWN * core, OWN), OWN)
    mate_rows = pl.ds(pl.multiple_of(OWN * (1 - core), OWN), OWN)

    def part_copy(n):
        return pltpu.make_async_remote_copy(src_ref=acc_s.at[n % 4, mate_rows, :], dst_ref=got_s.at[n], send_sem=o_send.at[n], recv_sem=o_recv.at[n],
                                            device_id={"sp": mate}, device_id_type=MESH)

    def y_copy(n):
        return pltpu.make_async_copy(out_s.at[n % 4], y_ref.at[:, pl.ds(pl.multiple_of(2 * NARROW * n, 2 * NARROW), 2 * NARROW)], y_sem.at[n % 4])

    def finish(n):
        part_copy(n).wait_recv()
        here = pl.ds(pl.multiple_of(2 * NARROW * n, 2 * NARROW), 2 * NARROW)
        out_s[n % 4] = (x_s[:, here].astype(jnp.float32) + (acc_s[n % 4, own_rows, :] + got_s[n])).astype(jnp.bfloat16)
        y_copy(n).start()
        part_copy(n).wait_send()

    def outputs(t, _):
        for u in range(2):
            ready((2 * t + u + 4) % SLOTS)
        for u in range(2):
            n = 2 * t + u
            slot = (n + 4) % SLOTS
            for k in range(2):
                acc_s[n % 4, :, NARROW * k : NARROW * k + NARROW] = _dot(a_s[:, :HALF], w_s[slot, HALF * k : HALF * k + HALF, :], 1, 0)
            part_copy(n).start()

        @pl.when(t >= 3)
        def _():
            for u in range(2):
                y_copy(2 * t - 6 + u).wait()

        @pl.when(t >= 1)
        def _():
            for u in range(2):
                finish(2 * t - 2 + u)

    lax.fori_loop(0, 6, outputs, None)
    for n in (6, 7):
        y_copy(n).wait()
    for n in (10, 11):
        finish(n)
    for n in (8, 9, 10, 11):
        y_copy(n).wait()
    for copy in sent:
        copy.wait_send()


def _turns():
    half = HEAD // 2
    power = np.float32(THETA) ** (-np.arange(half, dtype=np.float32) / np.float32(half))
    angle = np.arange(CHIP * CHIPS, dtype=np.float32)[:, None] * power.astype(np.float32)
    return np.concatenate([np.cos(angle), np.sin(angle)], 1).astype(np.float32)


def solution(mesh):
    def step(x, gain, wq, wk, wv, wo):
        anywhere = pl.BlockSpec(memory_space=pl.ANY)
        f32, bf16, dma = jnp.float32, jnp.bfloat16, pltpu.SemaphoreType.DMA
        return pl.pallas_call(
            _kernel,
            out_shape=jax.ShapeDtypeStruct((OWN, D), bf16),
            in_specs=[anywhere] * 7,
            out_specs=anywhere,
            scratch_shapes=[
                pltpu.VMEM((SLOTS, D, NARROW), bf16),
                pltpu.VMEM((CHIP, D), bf16),
                pltpu.VMEM((OWN, D), bf16),
                pltpu.VMEM((1, D), f32),
                pltpu.VMEM((CHIP, HEAD), f32),
                pltpu.VMEM((CHIP, HEAD), f32),
                pltpu.VMEM((CHIPS, CHIP, 2 * KVW), bf16),
                pltpu.VMEM((Q_HEADS, CHIP, HEAD), bf16),
                pltpu.VMEM((KV_HEADS, HEAD + 8, COLS), f32),
                pltpu.VMEM((KV_HEADS, 1, COLS), f32),
                pltpu.VMEM((4, CHIP, 2 * NARROW), f32),
                pltpu.VMEM((12, OWN, 2 * NARROW), f32),
                pltpu.VMEM((4, OWN, 2 * NARROW), bf16),
                dma((SLOTS, 2)), dma((4,)), dma((2,)), dma((4,)), dma((4,)), dma((21,)), dma((CHIPS, 3)), dma((12,)), dma((12,)), dma((4,)),
            ],
            compiler_params=pltpu.CompilerParams(collective_id=0, has_side_effects=True, vmem_limit_bytes=67_043_328),
            cost_estimate=pl.CostEstimate(flops=26 * 10**9, bytes_accessed=92 * 10**6, transcendentals=13 * 10**6),
        )(x, gain.astype(f32).reshape(1, D), jnp.asarray(_turns()), wq, wk, wv, wo)

    tokens, whole = P(("dp", "sp"), None), P(None, None)
    return jax.shard_map(step, mesh=mesh, in_specs=(tokens, P(None), whole, whole, whole, whole), out_specs=tokens, check_vma=False)
```

```python
import functools

import jax
import jax.numpy as jnp
import numpy as np
from jax import lax
from jax.experimental import pallas as pl
from jax.experimental.pallas import tpu as pltpu
from jax.sharding import PartitionSpec as P

MESH = pl.DeviceIdType.MESH
HEAD = 128
THETA = 10000
NEG = -1e30
LOG2E = 1.4426950408889634
E = HEAD**-0.5 * LOG2E

OWN = 128
CHIP = 2 * OWN
D = 6144
CHIPS = 8
Q_HEADS, KV_HEADS = 24, 4
GROUP = Q_HEADS // KV_HEADS
COLS = GROUP * CHIP
WIDE = 512
SLOTS = 12
NARROW = 256
HALF = D // 2
KVW = KV_HEADS * HEAD
PIECES = ((0, 96), (96, 80), (176, 80))


def _dot(a, b, ca, cb):
    return lax.dot_general(a, b, (((ca,), (cb,)), ((), ())), preferred_element_type=jnp.float32)


def _xor(m, d):
    return sum(b * ((m // b) % 2 + (d // b) % 2 - 2 * ((m // b) % 2) * ((d // b) % 2)) for b in (1, 2, 4))


def _kernel(x_ref, gain_ref, turn_ref, wq_ref, wk_ref, wv_ref, wo_ref, y_ref,
            w_s, a_s, x_s, gain_s, turn_s, cos_s, sin_s, kv_s, q_s, mix_s, top_s, acc_s, got_s,
            w_sem, x_sem, t_sem, a_send, a_recv, kv_send, kv_recv, o_send, o_recv):
    me = lax.axis_index("sp")
    chip, core = me // 2, me % 2
    mate = 2 * chip + 1 - core
    nx, ny, nz = (_xor(chip, d) for d in (4, 2, 1))

    def load(i):
        slot = i % SLOTS
        if i < 16:
            ref, col = ((wk_ref, core * KVW + NARROW * i) if i < 2 else (wv_ref, core * KVW + NARROW * (i - 2)) if i < 4
                        else (wq_ref, core * HALF + NARROW * (i - 4)))
            col = pl.multiple_of(col, 128)
            return [pltpu.make_async_copy(ref.at[pl.ds(HALF * k, HALF), pl.ds(col, NARROW)],
                                          w_s.at[slot, pl.ds(HALF * k, HALF), :], w_sem.at[slot, k]) for k in range(2)]
        n = i - 16
        row = pl.multiple_of(core * HALF, 128)
        return [pltpu.make_async_copy(wo_ref.at[pl.ds(row, HALF), pl.ds(2 * NARROW * n + NARROW * k, NARROW)],
                                      w_s.at[slot, pl.ds(HALF * k, HALF), :], w_sem.at[slot, k]) for k in range(2)]

    def fetch(i):
        for copy in load(i):
            copy.start(priority=1)

    def ready(slot):
        for k in range(2):
            pltpu.make_async_copy(wo_ref.at[pl.ds(0, HALF), pl.ds(0, NARROW)], w_s.at[slot, pl.ds(HALF * k, HALF), :],
                                  w_sem.at[slot, k]).wait()

    rows = D // 192
    def x_copy(i):
        return pltpu.make_async_copy(x_ref.at[pl.ds(rows * i, rows), :], x_s.at[pl.ds(rows * i, rows), :], x_sem.at[i])

    tables = [pltpu.make_async_copy(gain_ref, gain_s, t_sem.at[0]),
              pltpu.make_async_copy(turn_ref, turn_s, t_sem.at[1])]
    tables[0].start()
    for i in range(OWN // rows):
        x_copy(i).start()
    for t in tables[1:]:
        t.start()
    for i in range(SLOTS):
        fetch(i)

    barrier = pltpu.get_barrier_semaphore()
    for to in (mate, 2 * nx + core, 2 * ny + core, 2 * nz + core):
        pl.semaphore_signal(barrier, inc=1, device_id={"sp": to}, device_id_type=MESH)
    pl.semaphore_wait(barrier, 4)

    def a_copy(i, first):
        part = pl.ds(pl.multiple_of(first + rows * i, rows), rows)
        return pltpu.make_async_remote_copy(src_ref=a_s.at[part, :], dst_ref=a_s.at[part, :], send_sem=a_send.at[i], recv_sem=a_recv.at[i],
                                            device_id={"sp": mate}, device_id_type=MESH)

    tables[0].wait()

    def norm(i, _):
        x_copy(i).wait()
        wide = x_s[pl.ds(pl.multiple_of(rows * i, rows), rows), :].astype(jnp.float32)
        scale = lax.rsqrt(jnp.mean(wide * wide, -1, keepdims=True) + 1e-6)
        gain = gain_s[...].astype(jnp.float32)
        for n in range(D // 128):
            a_s[pl.ds(pl.multiple_of(OWN * core + rows * i, rows), rows), 128 * n : 128 * n + 128] = (
                wide[:, 128 * n : 128 * n + 128] * scale * gain[n : n + 1, :]).astype(jnp.bfloat16)
        a_copy(i, OWN * core).start()

    lax.fori_loop(0, OWN // rows, norm, None)
    for t in tables[1:]:
        t.wait()
    for i in range(OWN // rows):
        a_copy(i, OWN * (1 - core)).wait_recv()
        a_copy(i, OWN * core).wait_send()
    cos_a, sin_a = (turn_s[n, pl.ds(CHIP + chip, 1), :] for n in range(2))
    cos_b, sin_b = (turn_s[n, :CHIP, :] for n in range(2))
    low = lax.broadcasted_iota(jnp.int32, (CHIP, HEAD), 1) < HEAD // 2
    sine = sin_a * cos_b + cos_a * sin_b
    cos_s[...] = cos_a * cos_b - sin_a * sin_b
    sin_s[...] = jnp.where(low, -sine, sine)

    def turned(t):
        t = t.astype(jnp.bfloat16).astype(jnp.float32)
        return (t * cos_s[...] + pltpu.roll(t, HEAD // 2, 1) * sin_s[...]).astype(jnp.bfloat16)

    for i in range(4):
        ready(i)
    for i in range(4):
        t = _dot(a_s[...], w_s[i], 1, 0)
        for n in range(2):
            head = t[:, HEAD * n : HEAD * n + HEAD]
            kv_s[chip, :, NARROW * i + HEAD * n : NARROW * i + HEAD * n + HEAD] = turned(head) if i < 2 else head.astype(jnp.bfloat16)
    for i in range(4):
        fetch(SLOTS + i)

    def kv_copy(source, p, to, sem):
        part = pl.ds(PIECES[p][0], PIECES[p][1])
        return pltpu.make_async_remote_copy(src_ref=kv_s.at[source, part, :], dst_ref=kv_s.at[source, part, :], send_sem=kv_send.at[sem],
                                            recv_sem=kv_recv.at[source, p], device_id={"sp": 2 * to + core}, device_id_type=MESH)

    def arrived(source, p):
        kv_copy(source, p, nx, 0).wait_recv()

    sent = []

    def send(source, p, to):
        copy = kv_copy(source, p, to, len(sent))
        copy.start()
        sent.append(copy)

    for k in range(3):
        for at, to in enumerate((nx, ny, nz)):
            send(chip, (at + k) % 3, to)

    def forward(k):
        for at, (source, to) in enumerate(((nx, ny), (ny, nz), (nz, nx))):
            arrived(source, (at + k) % 3)
            send(source, (at + k) % 3, to)

    def queries(t):
        first = (4 + 4 * t) % SLOTS
        for u in range(4):
            ready(first + u)
        for u in range(4):
            got = _dot(a_s[...], w_s[first + u], 1, 0)
            for n in range(2):
                q_s[8 * t + 2 * u + n] = turned(got[:, HEAD * n : HEAD * n + HEAD])

    queries(0)
    for i in range(4):
        fetch(16 + i)
    queries(1)
    for i in range(4):
        fetch(20 + i)
    forward(0)
    queries(2)
    for i in range(4):
        fetch(24 + i)
    forward(1)

    ones = jnp.ones((8, CHIP), jnp.bfloat16)

    pieces = [(h, at) for h in range(KV_HEADS) for at in range(0, COLS, WIDE)]

    def block(source, own):
        def scores(h, at):
            q = q_s[GROUP * h : GROUP * h + GROUP].reshape(COLS, HEAD)
            return _dot(kv_s[source, :, HEAD * h : HEAD * h + HEAD], q[at : at + WIDE], 1, 1)

        following = scores(*pieces[0])
        for i, (h, at) in enumerate(pieces):
            s = following
            if i + 1 < len(pieces):
                following = scores(*pieces[i + 1])
            if at == 0:
                values = jnp.concatenate([kv_s[source, :, KVW + HEAD * h : KVW + HEAD * h + HEAD].T, ones], axis=0)
            here = slice(at, at + WIDE)
            if own:
                query = lax.broadcasted_iota(jnp.int32, s.shape, 1) % CHIP
                s = jnp.where(query >= lax.broadcasted_iota(jnp.int32, s.shape, 0), s, 2 * NEG)
                top = s.max(axis=0, keepdims=True)
                top_s[h, :, here] = top
                mix_s[h, :, here] = _dot(values, jnp.exp2((s - top) * E).astype(jnp.bfloat16), 1, 0)
            else:
                old = top_s[h, :, here]
                top = jnp.maximum(old, s.max(axis=0, keepdims=True))
                top_s[h, :, here] = top
                p = jnp.exp2((s - top) * E).astype(jnp.bfloat16)
                mix_s[h, :, here] = mix_s[h, :, here] * jnp.exp2((old - top) * E) + _dot(values, p, 1, 0)

    block(chip, True)
    forward(2)

    def other(i, _):
        source = _xor(chip, i + 1 + i // 2 - 2 * (i // 3) + i // 6)

        @pl.when(source < chip)
        def _():
            block(source, False)

    far = [(_xor(chip, 6), 0, nz), (_xor(chip, 3), 1, nx), (_xor(chip, 5), 2, ny)]
    last = _xor(chip, 7)
    def step(i, _):
        @pl.when(i == 3)
        def _():
            for source, p, to in far:
                arrived(source, p)
                kv_copy(source, p, to, 18 + p).start()
            for source, p, to in far:
                for other_p in range(3):
                    if other_p != p:
                        arrived(source, other_p)

        @pl.when(i == 6)
        def _():
            for p in range(3):
                arrived(last, p)

        other(i, None)

    lax.fori_loop(0, 7, step, None)
    for source, p, to in far:
        sent.append(kv_copy(source, p, to, 18 + p))

    for h in range(KV_HEADS):
        for g in range(GROUP):
            here = slice(g * CHIP, g * CHIP + CHIP)
            seen = mix_s[h, :HEAD, here] * (1 / mix_s[h, HEAD : HEAD + 1, here])
            n = GROUP * h + g
            a_s[:, HEAD * n : HEAD * n + HEAD] = seen.T.astype(jnp.bfloat16)

    own_rows = pl.ds(pl.multiple_of(OWN * core, OWN), OWN)
    mate_rows = pl.ds(pl.multiple_of(OWN * (1 - core), OWN), OWN)

    def part_copy(n):
        return pltpu.make_async_remote_copy(src_ref=acc_s.at[n % 8, mate_rows, :], dst_ref=got_s.at[n], send_sem=o_send.at[n], recv_sem=o_recv.at[n],
                                            device_id={"sp": mate}, device_id_type=MESH)

    def finish(first):
        for n in range(first, first + 4):
            part_copy(n).wait_recv()
            part_copy(n).wait_send()
        for n in range(first, first + 4):
            here = slice(2 * NARROW * n, 2 * NARROW * n + 2 * NARROW)
            y_ref[:, here] = (x_s[:, here].astype(jnp.float32) + (acc_s[n % 8, own_rows, :] + got_s[n])).astype(jnp.bfloat16)

    for n in range(12):
        ready((n + 4) % SLOTS)
    for n in range(12):
        slot = (n + 4) % SLOTS
        for k in range(2):
            acc_s[n % 8, :, NARROW * k : NARROW * k + NARROW] = _dot(a_s[:, :HALF], w_s[slot, HALF * k : HALF * k + HALF, :], 1, 0)
        part_copy(n).start()
        if n in (7, 10):
            finish(0 if n == 7 else 4)
    finish(8)
    for copy in sent:
        copy.wait_send()


def _turns():
    half = HEAD // 2
    power = np.float64(THETA) ** (-np.arange(half) / half)
    place = np.concatenate([np.arange(CHIP), CHIP * np.arange(CHIPS)])
    angle = np.tile(place[:, None] * power, (1, 2))
    return np.stack([np.cos(angle), np.sin(angle)]).astype(np.float32)


def solution(mesh):
    def step(x, gain, wq, wk, wv, wo):
        anywhere = pl.BlockSpec(memory_space=pl.ANY)
        f32, bf16, dma = jnp.float32, jnp.bfloat16, pltpu.SemaphoreType.DMA
        return pl.pallas_call(
            _kernel,
            out_shape=pltpu.VMEM((OWN, D), bf16),
            in_specs=[anywhere] * 7,
            out_specs=pl.BlockSpec(memory_space=pltpu.VMEM),
            scratch_shapes=[
                pltpu.VMEM((SLOTS, D, NARROW), bf16),
                pltpu.VMEM((CHIP, D), bf16),
                pltpu.VMEM((OWN, D), bf16),
                pltpu.VMEM((D // 128, 128), bf16),
                pltpu.VMEM((2, CHIP + CHIPS, HEAD), f32),
                pltpu.VMEM((CHIP, HEAD), f32),
                pltpu.VMEM((CHIP, HEAD), f32),
                pltpu.VMEM((CHIPS, CHIP, 2 * KVW), bf16),
                pltpu.VMEM((Q_HEADS, CHIP, HEAD), bf16),
                pltpu.VMEM((KV_HEADS, HEAD + 8, COLS), f32),
                pltpu.VMEM((KV_HEADS, 1, COLS), f32),
                pltpu.VMEM((8, CHIP, 2 * NARROW), f32),
                pltpu.VMEM((12, OWN, 2 * NARROW), f32),
                dma((SLOTS, 2)), dma((4,)), dma((2,)), dma((4,)), dma((4,)), dma((21,)), dma((CHIPS, 3)), dma((12,)), dma((12,)),
            ],
            compiler_params=pltpu.CompilerParams(collective_id=0, has_side_effects=True, vmem_limit_bytes=65_400_000),
            cost_estimate=pl.CostEstimate(flops=26 * 10**9, bytes_accessed=92 * 10**6, transcendentals=13 * 10**6),
        )(x, gain.reshape(D // 128, 128), jnp.asarray(_turns()), wq, wk, wv, wo)

    tokens, whole = P(("dp", "sp"), None), P(None, None)
    return jax.shard_map(step, mesh=mesh, in_specs=(tokens, P(None), whole, whole, whole, whole), out_specs=tokens, check_vma=False)
```
